32 devices in a mesh: row: 4 (over y, core), col: 8 (over z, x).
Axes of the slice: x: 2, y: 2, z: 4, core: 2. Of those that a mesh axis runs over, the one named last changes fastest.
Arguments:
- constraint: bfloat16 [8192, 16384], P('row', 'col'), may hold values from -0.046875 to 0.046875
- pattern: int32 [64, 128], P('row', 'col'), may hold values 0 or 1
- objective: float32 [16384, 256], P('col'), may hold values from -31 to 31
- row_bound: float32 [8192, 256], P('row'), may hold values from -31 to 31
- lower_bound: float32 [16384], P('col'), may hold values from -2 to -0.5
- upper_bound: float32 [16384], P('col'), may hold values from 0.5 to 2
Outputs:
- primal: float32 [16384, 256], P('col')
- dual_values: float32 [8192, 256], P('row')
- residual_norms: float32 [256], replicated
The draws below stay inside these ranges and needn't reach their ends.
All inputs are finite; a program needn't handle non-finite values. No bound on the sum of `pattern` on one device may be relied on, other than what follows from the above.
Results may differ from the reference program's by a relative error of at most 0.0019.
Values may be sent and summed in bfloat16 or wider, within the bound.
No kernel may reach another device: no remote copies, remote signals or barrier semaphores. Data moves between devices by JAX's collectives and lax.ppermute only.
A program may use at most 128 MiB of HBM per device.

```python
import jax
import jax.numpy as jnp
from jax import lax

BLOCK = 128
K = 256
ITERS = 3
MB = 64
NB = 128
M = 8192
N = 16384


def ramped(key, length, columns):
    first, second = jax.random.split(key)
    ramp_scale = 1.0 + 2.0 * jnp.arange(length, dtype=jnp.float32) / (length - 1)
    rough_scale = jnp.exp(jax.random.uniform(second, (length, 1), jnp.float32, -0.7, 0.7))
    base_values = jnp.clip(jax.random.normal(first, (length, columns), jnp.float32), -5.0, 5.0)
    return base_values * ramp_scale[:, None] * rough_scale


def draw_objective(key, part):
    return ramped(jax.random.fold_in(key, 11), N, K)


def draw_row_bound(key, part):
    return ramped(jax.random.fold_in(key, 23), M, K)


def with_ends(drawn, rng, low, top_value):
    place = [jax.random.randint(jax.random.fold_in(rng, axis), (), 0, length) for axis, length in enumerate(drawn.shape)]
    longest = drawn.shape.index(max(drawn.shape))
    next_to = place[:longest] + [(place[longest] + 1) % drawn.shape[longest]] + place[longest + 1:]
    return drawn.at[tuple(place)].set(low).at[tuple(next_to)].set(top_value)


def level_of(own_key, shape, cuts, low, top_value):
    loudness, own = 1.0, jax.random.fold_in(own_key, 6)
    for dim, shards_of in cuts:
        draws = jnp.exp(jax.random.uniform(jax.random.fold_in(own, dim), (shards_of,), jnp.float32, low / len(cuts), top_value / len(cuts)))
        loudness = loudness * jnp.repeat(draws, shape[dim] // shards_of).reshape([-1 if axis == dim else 1 for axis in range(len(shape))])
    return loudness


def noise(stream_key, extent, scale, bound, cuts=(), kind=jnp.bfloat16):
    drawn = scale * jax.random.normal(stream_key, extent, jnp.float32)
    if cuts:
        drawn = drawn * level_of(stream_key, extent, cuts, -0.22, 0.18)
    return jnp.clip(drawn, -bound, bound).astype(kind)


def setup_inputs(seed: int = 0) -> dict:
    arg_keys = jax.random.split(jax.random.key(seed), 7)
    constraint = noise(arg_keys[0], (M, N), N ** -0.5, 0.046875, ((0, 4), (1, 8)))
    pattern = with_ends((jax.random.randint(arg_keys[1], (MB, NB), 0, 4) < 3).astype(jnp.int32), jax.random.fold_in(arg_keys[1], 1), 0, 1)
    objective = draw_objective(jax.random.fold_in(arg_keys[6], 71), 0)
    row_bound = draw_row_bound(jax.random.fold_in(arg_keys[6], 71), 0)
    lower_bound = jnp.clip(-2.0 + 1.5 * jax.random.uniform(arg_keys[4], (N,), jnp.float32) ** level_of(arg_keys[4], (N,), ((0, 8),), -0.2, 0.2), -2.0, -0.5)
    upper_bound = jnp.clip(0.5 + 1.5 * jax.random.uniform(arg_keys[5], (N,), jnp.float32) ** level_of(arg_keys[5], (N,), ((0, 8),), -0.2, 0.2), 0.5, 2.0)
    return {"constraint": constraint, "pattern": pattern, "objective": objective, "row_bound": row_bound, "lower_bound": lower_bound, "upper_bound": upper_bound}


step_primal = 0.6
step_dual = 0.6
epsilon = 1e-06

def reference(constraint, pattern, objective, row_bound, lower_bound, upper_bound):
    row_blocks, col_blocks = pattern.shape
    matrix = (constraint.reshape(row_blocks, BLOCK, col_blocks, BLOCK) * pattern.astype(jnp.bfloat16)[:, None, :, None]).reshape(row_blocks * BLOCK, col_blocks * BLOCK)
    primal = jnp.zeros((col_blocks * BLOCK, K), jnp.float32)
    dual_values = jnp.zeros((row_blocks * BLOCK, K), jnp.float32)
    residual_norms = jnp.zeros((K,), jnp.float32)
    for iteration in range(ITERS):
        if iteration == 0:
            gradient = objective
        else:
            gradient = objective - jnp.dot(matrix.T, dual_values.astype(jnp.bfloat16), preferred_element_type=jnp.float32)
        updated = jnp.clip(primal - step_primal * gradient, lower_bound[:, None], upper_bound[:, None])
        extrapolated = (2.0 * updated - primal).astype(jnp.bfloat16)
        slack_rows = row_bound - jnp.dot(matrix, extrapolated, preferred_element_type=jnp.float32)
        dual_values = jnp.maximum(dual_values + step_dual * slack_rows, 0.0)
        violation = lax.optimization_barrier(jnp.sum(jnp.maximum(slack_rows, 0.0) ** 2, axis=0))
        movement = lax.optimization_barrier(jnp.sum((updated - primal) ** 2, axis=0))
        residual_norms = residual_norms + jnp.sqrt(violation / M + epsilon) + jnp.sqrt(movement / N + epsilon)
        primal = updated
    return (primal, dual_values, residual_norms)
```

```python
import functools

import jax
import jax.numpy as jnp
from jax import lax
from jax.experimental import pallas as pl
from jax.experimental.pallas import tpu as pltpu
from jax.sharding import PartitionSpec as P

BLOCK = 128
LANES = 128
ITERS = 3

step_primal = 0.6
step_dual = 0.6
epsilon = 1e-06


def bits_of(size):
    bits = size.bit_length() - 1
    assert size == 1 << bits
    return bits


def exchange(value, axis, bit):
    size = lax.axis_size(axis)
    return lax.ppermute(value, axis, [(i, i ^ (1 << bit)) for i in range(size)])


def rounded_bf16(value):
    return lax.reduce_precision(value, exponent_bits=8, mantissa_bits=7)


def mask_kernel(place_ref, pattern_ref, block_ref, out_ref, *, half, share, width):
    position = half * pl.num_programs(0) + pl.program_id(0)
    row_start = (position ^ place_ref[0]) * share
    col_start = (pl.program_id(1) ^ place_ref[1]) * (width // BLOCK)
    rows = min(share, BLOCK)
    for r in range(share // rows):
        pattern_row = (row_start + r * rows) // BLOCK
        for c in range(width // BLOCK):
            present = pattern_ref[pattern_row, col_start + c]
            tile = block_ref[r * rows : (r + 1) * rows, c * BLOCK : (c + 1) * BLOCK]
            out_ref[r * rows : (r + 1) * rows, c * BLOCK : (c + 1) * BLOCK] = jnp.where(
                present != 0, tile, jnp.zeros_like(tile)
            )


def masked_half(constraint, pattern, place, half, positions):
    local_rows, local_cols = constraint.shape
    share = local_rows // positions
    width = local_cols // 2
    count = positions // 2

    def source(j, h, place_ref, pattern_ref):
        return ((half * count + j) ^ place_ref[0], h ^ place_ref[1])

    return pl.pallas_call(
        functools.partial(mask_kernel, half=half, share=share, width=width),
        grid_spec=pltpu.PrefetchScalarGridSpec(
            num_scalar_prefetch=2,
            grid=(count, 2),
            in_specs=[pl.BlockSpec((share, width), source)],
            out_specs=pl.BlockSpec((share, width), lambda j, h, a, b: (j, h)),
        ),
        out_shape=jax.ShapeDtypeStruct((local_rows // 2, local_cols), constraint.dtype),
        name=f"mask_half{half}",
    )(place, pattern, constraint)


def on_device(constraint, pattern, objective, row_bound, lower_bound, upper_bound):
    local_rows, local_cols = constraint.shape
    batch = objective.shape[1]
    row_devices = lax.axis_size("row")
    col_devices = lax.axis_size("col")
    row_bits = bits_of(row_devices)
    col_bits = bits_of(col_devices)
    total_rows = local_rows * row_devices
    total_cols = local_cols * col_devices
    share = local_rows // col_devices
    half_cols = local_cols // 2
    core = lax.axis_index("row") & 1
    col_index = lax.axis_index("col")
    reverse = jnp.int32(0)
    for b in range(col_bits):
        reverse = reverse | (((col_index >> b) & 1) << (col_bits - 1 - b))
    place = jnp.stack([reverse, core]).astype(jnp.int32)
    order = jnp.arange(col_devices, dtype=jnp.int32) ^ reverse

    upper_half = masked_half(constraint, pattern, place, 1, col_devices)
    lower_half = masked_half(constraint, pattern, place, 0, col_devices)

    bound_rows = row_bound.reshape(col_devices, share, batch)[order].reshape(local_rows, batch)

    def halves(value):
        first = lax.dynamic_slice_in_dim(value, core * half_cols, half_cols, 0)
        second = lax.dynamic_slice_in_dim(value, (1 - core) * half_cols, half_cols, 0)
        return first, second

    objective_own, objective_other = halves(objective)
    lower_own, lower_other = halves(lower_bound[:, None])
    upper_own, upper_other = halves(upper_bound[:, None])

    chunks = [slice(c * LANES, (c + 1) * LANES) for c in range(batch // LANES)]
    states = []
    for c in chunks:
        states.append({"c": c, "primal": None, "dual": None, "movement": [], "violation": []})

    def forward(state):
        extrapolated = state["extrapolated"]
        send = jnp.dot(upper_half, extrapolated, preferred_element_type=jnp.float32).astype(jnp.bfloat16)
        keep = jnp.dot(lower_half, extrapolated, preferred_element_type=jnp.float32)
        for b in range(col_bits):
            received = exchange(send, "col", b)
            total = keep + received.astype(jnp.float32)
            if b + 1 < col_bits:
                middle = total.shape[0] // 2
                send = total[middle:].astype(jnp.bfloat16)
                keep = total[:middle]
        gathered = rounded_bf16(total).astype(jnp.bfloat16)
        for b in reversed(range(col_bits)):
            gathered = jnp.concatenate([gathered, exchange(gathered, "col", b)], axis=0)
        slack = bound_rows[:, state["c"]] - gathered.astype(jnp.float32)
        old = state["dual"]
        state["dual"] = jnp.maximum(step_dual * slack if old is None else old + step_dual * slack, 0.0)
        state["violation"].append(jnp.sum(jnp.maximum(slack, 0.0) ** 2, axis=0))

    def backward(state):
        rounded = state["dual"].astype(jnp.bfloat16)
        middle = local_rows // 2
        dims = (((0,), (0,)), ((), ()))
        partial = lax.dot_general(
            lower_half, rounded[:middle], dims, preferred_element_type=jnp.float32
        ) + lax.dot_general(upper_half, rounded[middle:], dims, preferred_element_type=jnp.float32)
        own = partial[:half_cols] + exchange(partial[half_cols:], "row", 0)
        for b in range(1, row_bits):
            own = rounded_bf16(own)
            own = own + exchange(own.astype(jnp.bfloat16), "row", b).astype(jnp.float32)
        return objective_own[:, state["c"]] - own

    for iteration in range(ITERS):
        for state in states:
            if iteration == 0:
                updated = jnp.clip(-step_primal * objective_own[:, state["c"]], lower_own, upper_own)
                other = jnp.clip(-step_primal * objective_other[:, state["c"]], lower_other, upper_other)
                displacement = updated
                extrapolated = (2.0 * updated).astype(jnp.bfloat16)
                received = (2.0 * other).astype(jnp.bfloat16)
            else:
                gradient = backward(state)
                updated = jnp.clip(state["primal"] - step_primal * gradient, lower_own, upper_own)
                displacement = updated - state["primal"]
                extrapolated = (2.0 * updated - state["primal"]).astype(jnp.bfloat16)
                received = exchange(extrapolated, "row", 0)
            state["extrapolated"] = jnp.concatenate([extrapolated, received], axis=0)
            state["movement"].append(jnp.sum(displacement**2, axis=0))
            state["primal"] = updated
            forward(state)

    movement = jnp.stack([jnp.concatenate([s["movement"][i] for s in states]) for i in range(ITERS)])
    for b in range(col_bits):
        movement = movement + exchange(movement, "col", b)
    movement = movement + exchange(movement, "row", 0)
    violation = jnp.stack([jnp.concatenate([s["violation"][i] for s in states]) for i in range(ITERS)])
    for b in range(row_bits):
        violation = violation + exchange(violation, "row", b)
    residual_norms = jnp.zeros((batch,), jnp.float32)
    for iteration in range(ITERS):
        residual_norms = (
            residual_norms
            + jnp.sqrt(violation[iteration] / total_rows + epsilon)
            + jnp.sqrt(movement[iteration] / total_cols + epsilon)
        )

    primal_own = jnp.concatenate([s["primal"] for s in states], axis=1)
    primal_other = exchange(primal_own, "row", 0)
    primal = jnp.where(
        core == 0,
        jnp.concatenate([primal_own, primal_other], axis=0),
        jnp.concatenate([primal_other, primal_own], axis=0),
    )
    dual = jnp.concatenate([s["dual"] for s in states], axis=1)
    dual = dual.reshape(col_devices, share, batch)[order].reshape(local_rows, batch)
    return (primal, dual, residual_norms)


def solution(mesh):
    placed = (P("row", "col"), P("row", "col"), P("col", None), P("row", None), P("col"), P("col"))
    return jax.shard_map(
        on_device,
        mesh=mesh,
        in_specs=placed,
        out_specs=(P("col", None), P("row", None), P()),
        check_vma=False,
    )
```

```python
import jax
import jax.numpy as jnp
from jax import lax
from jax.experimental import pallas as pl
from jax.experimental.pallas import tpu as pltpu
from jax.sharding import PartitionSpec as P


BLOCK = 128
ITERS = 3
DIRECT_BITS = 2
MASK_ROWS = 256

step_primal = 0.6
step_dual = 0.6
epsilon = 1e-06

F32 = jnp.float32
BF16 = jnp.bfloat16


def bits_of(size):
    bits = size.bit_length() - 1
    assert size == 1 << bits
    return bits


def exchange(value, axis, distance):
    size = lax.axis_size(axis)
    return lax.ppermute(value, axis, [(i, i ^ distance) for i in range(size)])


def apart(*values):
    return lax.optimization_barrier(values)


def mask_kernel(half_ref, present_ref, block_ref, out_ref):
    rows = block_ref.shape[0]
    for r in range(rows // BLOCK):
        window = slice(r * BLOCK, (r + 1) * BLOCK)
        out_ref[window, :] = block_ref[window, :] * present_ref[0, r : r + 1, :]


def masked_half(constraint, present, half):
    local_rows, cols = constraint.shape
    rows = min(MASK_ROWS, local_rows // 2)
    steps = local_rows // 2 // rows
    source = lambda j, half: (half[0] * steps + j, 0)
    return pl.pallas_call(
        mask_kernel,
        grid_spec=pltpu.PrefetchScalarGridSpec(
            num_scalar_prefetch=1,
            grid=(steps,),
            in_specs=[
                pl.BlockSpec((1, rows // BLOCK, cols), lambda j, half: (half[0] * steps + j, 0, 0)),
                pl.BlockSpec((rows, cols), source),
            ],
            out_specs=pl.BlockSpec((rows, cols), lambda j, half: (j, 0)),
        ),
        out_shape=jax.ShapeDtypeStruct((local_rows // 2, cols), constraint.dtype),
        compiler_params=pltpu.CompilerParams(vmem_limit_bytes=8 << 20),
        name="mask",
    )(half.astype(jnp.int32)[None], present, constraint)


def presence(pattern, dtype):
    rows, cols = pattern.shape
    wide = jnp.broadcast_to(pattern.astype(dtype)[:, :, None], (rows, cols, BLOCK))
    return wide.reshape(rows * BLOCK // MASK_ROWS, MASK_ROWS // BLOCK, cols * BLOCK)


def in_place(pieces, block, bits):
    for d in range(bits):
        swap = ((block >> d) & 1) == 1
        pieces = [jnp.where(swap, pieces[t ^ (1 << d)], pieces[t]) for t in range(len(pieces))]
    return pieces


def spread_kernel(where_ref, *refs):
    (mine, other), out, sems = refs[:2], refs[-2], refs[-1]
    rows, lanes = mine.shape
    first = pl.multiple_of(where_ref[1], 8)
    copies = []
    for i, value in enumerate((mine, other)):
        left = pl.multiple_of((where_ref[0] ^ i) * lanes, lanes)
        copies.append(pltpu.make_async_copy(value, out.at[pl.ds(first, rows), pl.ds(left, lanes)], sems.at[i]))
    for copy in copies:
        copy.start()
    for copy in copies:
        copy.wait()


def spread(core, first, mine, other, shape, whole=None):
    anywhere = pl.BlockSpec(memory_space=pl.ANY)
    vmem = pl.BlockSpec(memory_space=pltpu.VMEM)
    where = jnp.stack([core, first]).astype(jnp.int32)
    inputs = [where, mine, other] + ([] if whole is None else [whole])
    return pl.pallas_call(
        spread_kernel,
        in_specs=[pl.BlockSpec(memory_space=pltpu.SMEM), vmem, vmem] + [anywhere] * (len(inputs) - 3),
        out_specs=anywhere,
        out_shape=jax.ShapeDtypeStruct(shape, F32),
        scratch_shapes=[pltpu.SemaphoreType.DMA((2,))],
        input_output_aliases={} if whole is None else {3: 0},
        compiler_params=pltpu.CompilerParams(vmem_limit_bytes=8 << 20),
        name="spread",
    )(*inputs)


def product(a, b):
    return jnp.dot(a, b, preferred_element_type=F32)


def transposed(a, b):
    return lax.dot_general(a, b, (((0,), (0,)), ((), ())), preferred_element_type=F32)


def iterations(constraint, pattern, objective, row_bound, lower_bound, upper_bound):
    local_rows, local_cols = constraint.shape
    batch = objective.shape[1]
    lanes = batch // 2
    row_devices = lax.axis_size("row")
    col_devices = lax.axis_size("col")
    row_bits = bits_of(row_devices)
    col_bits = bits_of(col_devices)
    total_rows = local_rows * row_devices
    total_cols = local_cols * col_devices
    half_rows = local_rows // 2
    share = local_rows // col_devices
    core = lax.axis_index("row") & 1
    col_index = lax.axis_index("col")
    bit = [(col_index >> b) & 1 for b in range(col_bits)]
    direct = range(max(1, col_bits - DIRECT_BITS), col_bits)
    halving = range(1, direct.start)
    peers = range(1, 1 << len(direct))
    block = sum(bit[b] << (col_bits - 1 - b) for b in direct)
    share_start = sum(bit[b] * (local_rows >> (b + 1)) for b in range(col_bits))
    halves = (bit[0] * half_rows, (1 - bit[0]) * half_rows)

    def distance(m):
        return sum(((m >> (col_bits - 1 - b)) & 1) << b for b in direct)

    lower = lower_bound[:, None]
    upper = upper_bound[:, None]

    def my_programs(value):
        return lax.dynamic_slice(value, (0, core * lanes), (value.shape[0], lanes))

    def their_programs(value):
        return lax.dynamic_slice(value, (0, (1 - core) * lanes), (value.shape[0], lanes))

    def first_step(cost):
        return (2.0 * jnp.clip(-step_primal * cost, lower, upper)).astype(BF16)

    send, received = [None] * 2, [None] * 2
    upper_rows, lower_rows = [None] * 2, [None] * 2
    own_presence = presence(pattern, constraint.dtype)
    upper_rows[0] = masked_half(constraint, own_presence, 1 - bit[0])
    wanted = my_programs(objective)
    (start,) = apart(first_step(wanted))
    (other_start,) = apart(first_step(their_programs(objective)))
    (send[0],) = apart(product(upper_rows[0], start).astype(BF16))
    received[0] = exchange(send[0], "col", 1)
    (theirs,) = apart(product(upper_rows[0], other_start).astype(BF16))
    send[1] = exchange(theirs, "row", 1)
    patterns = [pattern, exchange(pattern, "row", 1)]
    constraints = [constraint, exchange(constraint, "row", 1)]
    lower_rows[0] = masked_half(constraint, own_presence, bit[0])
    (theirs,) = apart(product(lower_rows[0], other_start))
    keep = [None, exchange(theirs, "row", 1)]
    (keep[0],) = apart(product(lower_rows[0], start))
    mine, theirs = apart(my_programs(row_bound), their_programs(row_bound))
    bound = [mine, exchange(theirs, "row", 1)]
    other_presence = presence(patterns[1], constraint.dtype)
    lower_rows[1] = masked_half(constraints[1], other_presence, bit[0])
    upper_rows[1] = masked_half(constraints[1], other_presence, 1 - bit[0])
    bound = list(apart(*bound))
    bound_half = [[lax.dynamic_slice_in_dim(bound[p], halves[h], half_rows, 0) for h in range(2)] for p in range(2)]
    bound_share = [lax.dynamic_slice_in_dim(bound[p], share_start, share, 0) for p in range(2)]
    wanted, *flat = apart(wanted, *bound_half[0], *bound_half[1], *bound_share)
    bound_half, bound_share = [flat[0:2], flat[2:4]], flat[4:]
    primal = None
    dual = [[None] * 2, [None] * 2]
    partial = None
    movement, violation = [], []
    joined = None

    def dual_step(old, slack):
        return jnp.maximum(step_dual * slack if old is None else old + step_dual * slack, 0.0)

    for iteration in range(ITERS):
        last = iteration + 1 == ITERS
        if iteration == 0:
            received[1] = exchange(send[1], "col", 1)
        else:
            for p in range(2):
                slack = bound_half[p][1] - received[p].astype(F32)
                dual[p][1] = dual_step(dual[p][1], slack)
                rounded = dual[p][1].astype(BF16)
                (more,) = apart(transposed(upper_rows[p], rounded))
                if p == 0:
                    (partial,) = apart(partial + more)
                else:
                    (partial,) = apart((partial + more).astype(BF16))
            own = partial
            for b in range(1, row_bits):
                arrived = exchange(own, "row", 1 << b)
                total = own.astype(F32) + arrived.astype(F32)
                if b + 1 < row_bits:
                    (own,) = apart(total.astype(BF16))
            if row_bits == 1:
                total = own.astype(F32)
            old = primal
            if old is None:
                old = jnp.clip(-step_primal * wanted, lower, upper)
            updated = jnp.clip(old - step_primal * (wanted - total), lower, upper)
            extrapolated = (2.0 * updated - old).astype(BF16)
            primal, old, extrapolated = apart(updated, old, extrapolated)
            for p in range(2):
                (send[p],) = apart(product(upper_rows[p], extrapolated).astype(BF16))
                received[p] = exchange(send[p], "col", 1)
            for p in range(2):
                (keep[p],) = apart(product(lower_rows[p], extrapolated))
            new, old, _ = apart(primal, old, keep[1])
            if iteration == 1:
                movement.append(jnp.sum(old**2, axis=0))
            movement.append(jnp.sum((new - old) ** 2, axis=0))
        total = jnp.stack([keep[p] + received[p].astype(F32) for p in range(2)])
        for b in halving:
            middle = total.shape[1] // 2
            away = lax.dynamic_slice_in_dim(total, (1 - bit[b]) * middle, middle, 1).astype(BF16)
            stay = lax.dynamic_slice_in_dim(total, bit[b] * middle, middle, 1)
            total = stay + exchange(away, "col", 1 << b).astype(F32)
        pieces = [
            jnp.stack(
                [
                    lax.dynamic_slice_in_dim(total[p], (block ^ m) * share, share, 0)
                    for p in range(2)
                ]
            )
            for m in range(1 + len(peers))
        ]
        stay, *pieces = apart(pieces[0], *(piece.astype(BF16) for piece in pieces[1:]))
        arrived = [exchange(piece, "col", distance(m)) for m, piece in zip(peers, pieces)]
        for piece in arrived:
            stay = stay + piece.astype(F32)
        slack = jnp.stack(bound_share) - stay
        violation.append(jnp.sum(jnp.maximum(slack, 0.0) ** 2, axis=(0, 1)))
        (mine,) = apart(stay.astype(BF16))
        pieces = [mine] + [exchange(mine, "col", distance(m)) for m in peers]
        pieces = in_place(pieces, block, len(direct))
        joined = list(apart(*(jnp.concatenate([piece[p] for piece in pieces], axis=0) for p in range(2))))
        for b in reversed(halving):
            both = jnp.stack(joined)
            other = exchange(both, "col", 1 << b)
            first = jnp.where(bit[b] == 0, both, other)
            second = jnp.where(bit[b] == 0, other, both)
            joined = list(jnp.concatenate([first, second], axis=1))
        for p in range(2):
            received[p] = exchange(joined[p], "col", 1)
        for p in range(2):
            slack = bound_half[p][0] - joined[p].astype(F32)
            dual[p][0] = dual_step(dual[p][0], slack)
            rounded = dual[p][0].astype(BF16)
            if not last:
                (more,) = apart(transposed(lower_rows[p], rounded))
                partial = more if p == 0 else partial + more

    (stats,) = apart(jnp.stack([*movement, *violation]))
    for b in [*halving, 0]:
        stats = stats + exchange(stats, "col", 1 << b)
    (stats,) = apart(stats)
    terms = [stats] + [exchange(stats, "col", distance(m)) for m in peers]
    while len(terms) > 1:
        terms = [terms[i] + terms[i + 1] for i in range(0, len(terms), 2)]
    (stats,) = terms
    moved, excess = stats[:ITERS], stats[ITERS:]
    for b in range(1, row_bits):
        excess = excess + exchange(excess, "row", 1 << b)
    norms = jnp.zeros((lanes,), F32)
    for iteration in range(ITERS):
        norms = (
            norms
            + jnp.sqrt(excess[iteration] / total_rows + epsilon)
            + jnp.sqrt(moved[iteration] / total_cols + epsilon)
        )
    other_norms = exchange(norms, "row", 1)
    other = exchange(primal, "row", 1)
    whole_primal = spread(core, 0, primal, other, (local_cols, batch))
    other = exchange(dual[1][0], "row", 1)
    whole_dual = spread(core, halves[0], dual[0][0], other, (local_rows, batch))
    whole_primal, whole_dual, *received = apart(whole_primal, whole_dual, *received)
    theirs = dual_step(dual[1][1], bound_half[1][1] - received[1].astype(F32))
    other = exchange(theirs, "row", 1)
    mine = dual_step(dual[0][1], bound_half[0][1] - received[0].astype(F32))
    whole_dual = spread(core, halves[1], mine, other, (local_rows, batch), whole_dual)
    residual_norms = jnp.where(core == 0, jnp.concatenate([norms, other_norms]), jnp.concatenate([other_norms, norms]))
    return (whole_primal, whole_dual, residual_norms)


def solution(mesh):
    placed = (P("row", "col"), P("row", "col"), P("col", None), P("row", None), P("col"), P("col"))
    return jax.shard_map(
        iterations,
        mesh=mesh,
        in_specs=placed,
        out_specs=(P("col", None), P("row", None), P()),
        check_vma=False,
    )
```
